32 devices in a mesh: ctx: 16 (over z, y, core), head: 2 (over x).
Axes of the slice: x: 2, y: 2, z: 4, core: 2. Of those that a mesh axis runs over, the one named last changes fastest.
Arguments:
- patch_hidden: bfloat16 [1024, 4096], P('ctx', 'head'), may hold values from -6 to 6
- queries: bfloat16 [1024, 32, 128], P('ctx', 'head'), may hold values from -6 to 6
- new_keys: bfloat16 [1024, 32, 128], P('ctx', 'head'), may hold values from -6 to 6
- new_values: bfloat16 [1024, 32, 128], P('ctx', 'head'), may hold values from -6 to 6
- cache_keys: bfloat16 [16384, 32, 128], P('ctx', 'head'), may hold values from -6 to 6
- cache_values: bfloat16 [16384, 32, 128], P('ctx', 'head'), may hold values from -6 to 6
- cache_request: int32 [16384], P('ctx'), may hold values from 0 to 7, never falling along the last dimension, each value on 1 to 4096 neighbouring positions
- new_request: int32 [1024], replicated, may hold values from 0 to 7, as said below
- out_weight: bfloat16 [32, 128, 4096], P('head'), may hold values from -0.375 to 0.375
- norm_gain: float32 [4096], replicated, may hold values from 0.1 to 1.9
- dec_kv_weight: bfloat16 [4096, 2, 1024], P(None, None, 'head'), may hold values from -0.09375 to 0.09375
- dec_query_weight: bfloat16 [1024, 1024], P(None, 'head'), may hold values from -0.1875 to 0.1875
- query_gain: float32 [64], replicated, may hold values from 0.1 to 1.9
- key_gain: float32 [64], replicated, may hold values from 0.1 to 1.9
- dec_out_weight: bfloat16 [1024, 1024], P('head'), may hold values from -0.75 to 0.75
- byte_states: bfloat16 [4096, 1024], P('ctx'), may hold values from -6 to 6
- byte_patch: int32 [4096], P('ctx'), may hold values from 0 to 1023, never falling along the last dimension, each value on 1 to 8 neighbouring positions
Outputs:
- patch_out: bfloat16 [1024, 4096], P('ctx', 'head')
- byte_out: bfloat16 [4096, 1024], P('ctx', 'head')
The draws below stay inside these ranges and needn't reach their ends.
Inputs may be any that keep to these rules, and one draw needn't show every extreme that they name: `new_request`: never falls along the patches; every request of 0 to 7 has an even number, two or more, of new patches. `cache_request`: never falls along the cached patches; every request has one or more cached patches. `byte_patch`: never falls along the bytes; every new patch owns one or more bytes.
All inputs are finite; a program needn't handle non-finite values.
Results may differ from the reference program's by a relative error of at most 0.017.
Values may be sent and summed in bfloat16 or wider, within the bound.
No kernel may reach another device: no remote copies, remote signals or barrier semaphores. Data moves between devices by JAX's collectives and lax.ppermute only.
A program may use at most 128 MiB of HBM per device.

```python
import math
import jax
import jax.numpy as jnp
import numpy as np
from jax import lax

D = 4096
H = 32
DH = 128
DD = 1024
DEC_H = 16
DEC_DH = 64
NEW_DEV = 64
NREQ = 8
P_SIZE = 1024
CTX = 16384
NBYTES = 4096


def request_cuts(key):
    lowest = max(1, min((P_SIZE // 2 + NEW_DEV) // 2, P_SIZE // 2 - NREQ - 1))
    chosen = jax.random.permutation(key, P_SIZE // 2 - lowest)[:NREQ - 1] + lowest
    return (jnp.sort(chosen) * 2).astype(jnp.int32)


def draw_new_request(key, part):
    cuts = request_cuts(jax.random.fold_in(key, 11))
    places = jnp.arange(P_SIZE, dtype=jnp.int32)
    return jnp.sum((places[:, None] >= cuts[None, :]).astype(jnp.int32), axis=1).astype(jnp.int32)


def draw_queries(key, part):
    base = jnp.clip(1.5 * jax.random.normal(jax.random.fold_in(key, 21), (P_SIZE, H, DH), jnp.float32), -6.0, 6.0)
    return base.astype(jnp.bfloat16)


def draw_new_keys(key, part):
    base = jnp.clip(jax.random.normal(jax.random.fold_in(key, 31), (P_SIZE, H, DH), jnp.float32), -6.0, 6.0)
    return base.astype(jnp.bfloat16)


def shard_levels(own_key, dims, pieces, smallest, top_value):
    def one(dim, parts):
        heights = jax.random.uniform(jax.random.fold_in(jax.random.fold_in(own_key, 6), dim), (parts,), jnp.float32, smallest / len(pieces), top_value / len(pieces))
        return jnp.repeat(jnp.exp(heights), dims[dim] // parts).reshape((-1,) + (1,) * (len(dims) - dim - 1))

    gain = one(*pieces[0])
    for cut in pieces[1:]:
        gain = gain * one(*cut)
    return gain


def split_up(count, total, bound, slope):
    weights = [(1 << 20) // math.isqrt(grade ** slope) + 1 for grade in range(2, count + 1)]
    spare, given = total - bound - (count - 1), [1] * (count - 1)
    while spare > 0:
        free = [i for i in range(count - 1) if given[i] < bound]
        pool, left = sum([weights[i] for i in free]), spare
        for i in free:
            more = min(bound - given[i], max(1, left * weights[i] // pool), spare)
            given[i] = given[i] + more
            spare = spare - more
    return np.array([bound] + given)


def uneven(own_key, count, total, reach, slope):
    if count == 2:
        one = jax.random.randint(own_key, (), max(1, total - reach), min(reach, total - 1) + 1)
        return jnp.stack([one, total - one])
    sizes = jnp.asarray(split_up(count, total, reach, slope), jnp.int32)
    twos = (count - 1) // 2
    donor, receiver = sizes[1:1 + 2 * twos:2], sizes[2:2 + 2 * twos:2]
    margin = jnp.minimum(donor - 1, reach - receiver)
    moved = jax.random.randint(jax.random.fold_in(own_key, 1), (twos,), 0, 1 << 20) % (margin + 1)
    sizes = sizes.at[1:1 + 2 * twos:2].set(donor - moved).at[2:2 + 2 * twos:2].set(receiver + moved)
    return sizes[jax.random.permutation(jax.random.fold_in(own_key, 2), count)]


def scatter_about(rng, shape, deviation, reach, split=(), held_as=jnp.bfloat16):
    gain = shard_levels(rng, shape, split, -0.22, 0.18) if split else 1.0
    entries = jax.random.normal(rng, shape, jnp.float32) * deviation * gain
    return jnp.minimum(jnp.maximum(entries, -reach), reach).astype(held_as)


def setup_inputs(seed: int = 0) -> dict:
    key_of = jax.random.split(jax.random.key(seed), 18)
    return {
        "patch_hidden": scatter_about(key_of[0], (P_SIZE, D), 1.0, 6.0, ((0, 16), (1, 2))),
        "queries": draw_queries(jax.random.fold_in(key_of[17], 71), 0),
        "new_keys": draw_new_keys(jax.random.fold_in(key_of[17], 71), 0),
        "new_values": scatter_about(key_of[3], (P_SIZE, H, DH), 1.0, 6.0, ((0, 16), (1, 2))),
        "cache_keys": scatter_about(key_of[4], (CTX, H, DH), 1.0, 6.0, ((0, 16), (1, 2))),
        "cache_values": scatter_about(key_of[5], (CTX, H, DH), 1.0, 6.0, ((0, 16), (1, 2))),
        "cache_request": jnp.searchsorted(jnp.cumsum(uneven(key_of[6], NREQ, CTX, CTX // 4, 2)), jnp.arange(CTX), side="right").astype(jnp.int32),
        "new_request": draw_new_request(jax.random.fold_in(key_of[17], 71), 0),
        "out_weight": scatter_about(key_of[8], (H, DH, D), (H * DH // 16) ** -0.5, 0.375, ((0, 2),)),
        "norm_gain": jnp.clip(1.0 + 0.18 * jax.random.normal(key_of[9], (D,), jnp.float32), 0.1, 1.9),
        "dec_kv_weight": scatter_about(key_of[10], (D, 2, DD), D ** -0.5, 0.09375, ((2, 2),)),
        "dec_query_weight": scatter_about(key_of[11], (DD, DD), DD ** -0.5, 0.1875, ((1, 2),)),
        "query_gain": jnp.clip(1.0 + 0.18 * jax.random.normal(key_of[12], (DEC_DH,), jnp.float32), 0.1, 1.9),
        "key_gain": jnp.clip(1.0 + 0.18 * jax.random.normal(key_of[13], (DEC_DH,), jnp.float32), 0.1, 1.9),
        "dec_out_weight": scatter_about(key_of[14], (DD, DD), (DD // 16) ** -0.5, 0.75, ((0, 2),)),
        "byte_states": scatter_about(key_of[15], (NBYTES, DD), 1.0, 6.0, ((0, 16),)),
        "byte_patch": jnp.searchsorted(jnp.cumsum(uneven(key_of[16], P_SIZE, NBYTES, 8, 2)), jnp.arange(NBYTES), side="right").astype(jnp.int32),
    }


def row_norm(values, gain_values, epsilon):
    meansq = lax.optimization_barrier(jnp.mean(values * values, axis=-1, keepdims=True))
    return values * lax.rsqrt(meansq + epsilon) * gain_values

def reference(patch_hidden, queries, new_keys, new_values, cache_keys, cache_values, cache_request, new_request, out_weight, norm_gain, dec_kv_weight, dec_query_weight, query_gain, key_gain, dec_out_weight, byte_states, byte_patch):
    query_index = jnp.arange(P_SIZE, dtype=jnp.int32)
    key_request = jnp.concatenate([cache_request.astype(jnp.int32), new_request.astype(jnp.int32)])
    key_position = jnp.concatenate([jnp.full((CTX,), -1, jnp.int32), query_index])
    visible = (key_request[None, :] == new_request[:, None]) & (key_position[None, :] <= query_index[:, None])
    all_keys = jnp.transpose(jnp.concatenate([cache_keys, new_keys], 0), (1, 0, 2))
    all_values = jnp.transpose(jnp.concatenate([cache_values, new_values], 0), (1, 0, 2))
    head_queries = jnp.transpose(queries, (1, 0, 2))

    def global_head(inputs):
        query_head, key_head, value_head = inputs
        scores = jnp.dot(query_head, key_head.T, preferred_element_type=jnp.float32) * DH ** (-0.5)
        highest = lax.optimization_barrier(jnp.max(jnp.where(visible, scores, -1e+30), axis=1, keepdims=True))
        weights = jnp.where(visible, jnp.exp(scores - highest), 0.0)
        totals = lax.optimization_barrier(jnp.sum(weights, axis=1, keepdims=True))
        mixed_rows = jnp.dot(weights.astype(jnp.bfloat16), value_head, preferred_element_type=jnp.float32)
        return (mixed_rows / totals).astype(jnp.bfloat16)
    attended = lax.map(global_head, (head_queries, all_keys, all_values))
    flattened = jnp.transpose(attended, (1, 0, 2)).reshape(P_SIZE, H * DH)
    projected = jnp.dot(flattened, out_weight.reshape(H * DH, D), preferred_element_type=jnp.float32)
    patch_out = (patch_hidden.astype(jnp.float32) + projected).astype(jnp.bfloat16)
    normed = row_norm(patch_out.astype(jnp.float32), norm_gain.astype(jnp.float32), 1e-05).astype(jnp.bfloat16)
    patch_proj = jnp.dot(normed, dec_kv_weight.reshape(D, 2 * DD), preferred_element_type=jnp.float32)
    patch_keys = row_norm(patch_proj[:, :DD].reshape(P_SIZE, DEC_H, DEC_DH), key_gain.astype(jnp.float32), 1e-06).astype(jnp.bfloat16)
    patch_values = patch_proj[:, DD:].astype(jnp.bfloat16).reshape(P_SIZE, DEC_H, DEC_DH)
    query_proj = jnp.dot(byte_states, dec_query_weight, preferred_element_type=jnp.float32).reshape(NBYTES, DEC_H, DEC_DH)
    byte_query = row_norm(query_proj, query_gain.astype(jnp.float32), 1e-06).astype(jnp.bfloat16)
    byte_request = new_request[byte_patch]
    seen = (new_request[None, :] == byte_request[:, None]) & (query_index[None, :] <= byte_patch[:, None])

    def byte_head(inputs):
        query_head, key_head, value_head = inputs
        scores = jnp.dot(query_head, key_head.T, preferred_element_type=jnp.float32) * DEC_DH ** (-0.5)
        weights = jnp.where(seen, jnp.exp(scores), 0.0)
        totals = lax.optimization_barrier(jnp.sum(weights, axis=1, keepdims=True))
        mixed_rows = jnp.dot(weights.astype(jnp.bfloat16), value_head, preferred_element_type=jnp.float32)
        return (mixed_rows / totals).astype(jnp.bfloat16)
    byte_mixed = lax.map(byte_head, (jnp.transpose(byte_query, (1, 0, 2)), jnp.transpose(patch_keys, (1, 0, 2)), jnp.transpose(patch_values, (1, 0, 2))))
    byte_flat = jnp.transpose(byte_mixed, (1, 0, 2)).reshape(NBYTES, DD)
    byte_terms = jnp.dot(byte_flat, dec_out_weight, preferred_element_type=jnp.float32)
    byte_out = (byte_states.astype(jnp.float32) + byte_terms).astype(jnp.bfloat16)
    return (patch_out, byte_out)
```

```python
import functools

import jax
import jax.numpy as jnp
from jax import lax
from jax.experimental import pallas as pl
from jax.experimental.pallas import tpu as pltpu
from jax.sharding import PartitionSpec as P

DEC_DH = 64
REQUESTS = 8
NEG = -float(2**100)
LOG2E = 1.4426950408889634
EXTRA = 8


def row_norm(values, gain_values, epsilon):
    meansq = jnp.mean(values * values, axis=-1, keepdims=True)
    return values * lax.rsqrt(meansq + epsilon) * gain_values


def pieces_of(value):
    high = value.astype(jnp.bfloat16)
    rest = value - high.astype(jnp.float32)
    middle = rest.astype(jnp.bfloat16)
    low = (rest - middle.astype(jnp.float32)).astype(jnp.bfloat16)
    zeros = jnp.zeros((EXTRA - 3,) + value.shape[1:], jnp.bfloat16)
    return jnp.concatenate([high, middle, low, zeros], axis=0)


def attention_kernel(
    chunk,
    scale,
    meta,
    q0,
    q1,
    qm,
    qpos,
    k0,
    k1,
    kn,
    km,
    knm,
    knpos,
    v0,
    v1,
    vn,
    out,
    m_ref,
    l_ref,
    acc_ref,
):
    dh = q0.shape[-1]
    rows = q0.shape[1]
    query = jnp.concatenate([q0[0], q1[0]], axis=0)
    query = jnp.concatenate([query, qm[...]], axis=1)
    m_ref[...] = jnp.full(m_ref.shape, 2.0 * NEG, jnp.float32)
    l_ref[...] = jnp.zeros(l_ref.shape, jnp.float32)
    acc_ref[...] = jnp.zeros(acc_ref.shape, jnp.float32)

    def step(scores, values):
        before = m_ref[...]
        now = jnp.maximum(before, jnp.max(scores, axis=0, keepdims=True))
        weights = jnp.exp2((scores - now) * scale)
        keep = jnp.exp2((before - now) * scale)
        m_ref[...] = now
        l_ref[...] = l_ref[...] * keep + jnp.sum(weights, axis=0, keepdims=True)
        mixed = jnp.dot(values, weights.astype(jnp.bfloat16), preferred_element_type=jnp.float32)
        acc_ref[...] = acc_ref[...] * keep + mixed

    def scores_of(keys, mask):
        return lax.dot_general(
            jnp.concatenate([keys, mask], axis=1),
            query,
            (((1,), (1,)), ((), ())),
            preferred_element_type=jnp.float32,
        )

    local = k0.shape[1]
    for which, (kref, vref) in enumerate(((k0, v0), (k1, v1))):
        for part in range(local // chunk):
            number = which * (local // chunk) + part
            low, high = meta[6 + 2 * number], meta[7 + 2 * number]

            @pl.when((low <= meta[1]) & (high >= meta[0]))
            def _():
                where = pl.ds(part * chunk, chunk)
                keys = kref[0, where, :]
                mask = km[pl.ds(number * chunk, chunk), :]
                step(scores_of(keys, mask), vref[0, :, where])

    @pl.when((meta[4] <= meta[1]) & (meta[5] >= meta[0]) & (meta[3] <= meta[2]))
    def _():
        scores = scores_of(kn[0], knm[...])
        scores = jnp.where(knpos[...] <= qpos[...], scores, NEG)
        step(scores, vn[0])

    total = l_ref[...]
    empty = total == 0.0
    total = jnp.where(empty, 1.0, total)
    mixed = (acc_ref[...] / total).astype(jnp.bfloat16)
    extra = pieces_of(m_ref[...] * scale + jnp.log2(total))
    for d in range(2):
        at = slice(d * rows, (d + 1) * rows)
        out[d, 0, :dh, :] = mixed[:, at]
        out[d, 0, dh:, :] = extra[:, at]


def attend(meta, q0, q1, qm, qpos, k0, k1, kn, km, knm, knpos, v0, v1, vn, chunk):
    heads, rows, dh = q0.shape
    scale = dh ** (-0.5) * LOG2E
    local, fresh = k0.shape[1], kn.shape[1]

    def per_head(*shape):
        return pl.BlockSpec((1,) + shape, lambda h, meta: (h, 0, 0))

    def whole(*shape):
        return pl.BlockSpec(shape, lambda h, meta: (0,) * len(shape))

    return pl.pallas_call(
        functools.partial(attention_kernel, chunk, scale),
        grid_spec=pltpu.PrefetchScalarGridSpec(
            num_scalar_prefetch=1,
            grid=(heads,),
            in_specs=[
                per_head(rows, dh),
                per_head(rows, dh),
                whole(*qm.shape),
                whole(*qpos.shape),
                per_head(local, dh),
                per_head(local, dh),
                per_head(fresh, dh),
                whole(*km.shape),
                whole(*knm.shape),
                whole(*knpos.shape),
                per_head(dh, local),
                per_head(dh, local),
                per_head(dh, fresh),
            ],
            out_specs=pl.BlockSpec((2, 1, dh + EXTRA, rows), lambda h, meta: (0, h, 0, 0)),
            scratch_shapes=[
                pltpu.VMEM((1, 2 * rows), jnp.float32),
                pltpu.VMEM((1, 2 * rows), jnp.float32),
                pltpu.VMEM((dh, 2 * rows), jnp.float32),
            ],
        ),
        out_shape=jax.ShapeDtypeStruct((2, heads, dh + EXTRA, rows), jnp.bfloat16),
        cost_estimate=pl.CostEstimate(
            flops=4 * heads * 2 * rows * (2 * local + fresh) * dh,
            bytes_accessed=4 * heads * 2 * local * dh,
            transcendentals=heads * 2 * rows * 2 * local,
        ),
        name="attend",
    )(meta, q0, q1, qm, qpos, k0, k1, kn, km, knm, knpos, v0, v1, vn)


def merge_kernel(a, b, out):
    dh = a.shape[1] - EXTRA
    for h in range(a.shape[0]):
        left = jnp.sum(a[h, dh : dh + 3, :].astype(jnp.float32), axis=0, keepdims=True)
        right = jnp.sum(b[h, dh : dh + 3, :].astype(jnp.float32), axis=0, keepdims=True)
        top = jnp.maximum(left, right)
        wl, wr = jnp.exp2(left - top), jnp.exp2(right - top)
        total = wl + wr
        scale = 1.0 / total
        mixed = a[h, :dh, :].astype(jnp.float32) * (wl * scale) + b[h, :dh, :].astype(
            jnp.float32
        ) * (wr * scale)
        out[h, :dh, :] = mixed.astype(jnp.bfloat16)
        out[h, dh:, :] = pieces_of(top + jnp.log2(total))


def merge(a, b):
    return pl.pallas_call(
        merge_kernel,
        out_shape=jax.ShapeDtypeStruct(a.shape, a.dtype),
        cost_estimate=pl.CostEstimate(
            flops=6 * a.size, bytes_accessed=6 * a.size, transcendentals=a.size // 64
        ),
        name="merge",
    )(a, b)


def byte_kernel(heads, blocks, meta, query, low, high, *refs):
    out = refs[blocks]
    rows = refs[0].shape[0]
    width = heads * DEC_DH
    total_rows = query.shape[0]
    lane = lax.broadcasted_iota(jnp.int32, (1, rows), 1)
    position = jnp.concatenate([lane + meta[b] * rows for b in range(blocks)], axis=1)
    seen = (position >= low[...]) & (position <= high[...])
    for h in range(heads):
        at = slice(h * DEC_DH, (h + 1) * DEC_DH)
        keys = jnp.concatenate([refs[b][:, at] for b in range(blocks)], axis=0)
        vat = slice(width + h * DEC_DH, width + (h + 1) * DEC_DH)
        values = jnp.concatenate([refs[b][:, vat] for b in range(blocks)], axis=0)
        scores = lax.dot_general(
            query[:, at], keys, (((1,), (1,)), ((), ())), preferred_element_type=jnp.float32
        )
        weights = jnp.where(seen, jnp.exp2(scores * (DEC_DH ** (-0.5) * LOG2E)), 0.0)
        total = jnp.sum(weights, axis=1, keepdims=True)
        mixed = jnp.dot(weights.astype(jnp.bfloat16), values, preferred_element_type=jnp.float32)
        out[:, at] = (mixed / total).astype(jnp.bfloat16)


def byte_attend(meta, query, low, high, blocks, heads):
    rows = query.shape[0]
    tile = min(rows, 256)
    width = heads * DEC_DH

    def whole(shape):
        return pl.BlockSpec(shape, lambda i, meta: (0,) * len(shape))

    return pl.pallas_call(
        functools.partial(byte_kernel, heads, len(blocks)),
        grid_spec=pltpu.PrefetchScalarGridSpec(
            num_scalar_prefetch=1,
            grid=(rows // tile,),
            in_specs=[
                pl.BlockSpec((tile, width), lambda i, meta: (i, 0)),
                pl.BlockSpec((tile, 1), lambda i, meta: (i, 0)),
                pl.BlockSpec((tile, 1), lambda i, meta: (i, 0)),
            ]
            + [whole(b.shape) for b in blocks],
            out_specs=pl.BlockSpec((tile, width), lambda i, meta: (i, 0)),
        ),
        out_shape=jax.ShapeDtypeStruct((rows, width), jnp.bfloat16),
        cost_estimate=pl.CostEstimate(
            flops=4 * rows * len(blocks) * blocks[0].shape[0] * width,
            bytes_accessed=2 * len(blocks) * blocks[0].size,
            transcendentals=rows * len(blocks) * blocks[0].shape[0] * heads,
        ),
        name="byte_attend",
    )(meta, query, low, high, *blocks)


def per_device(
    ctx,
    head,
    patch_hidden,
    queries,
    new_keys,
    new_values,
    cache_keys,
    cache_values,
    cache_request,
    new_request,
    out_weight,
    norm_gain,
    dec_kv_weight,
    dec_query_weight,
    query_gain,
    key_gain,
    dec_out_weight,
    byte_states,
    byte_patch,
):
    new_rows, local_heads, dh = queries.shape
    depth = ctx // 4
    half = local_heads // 2
    me = lax.axis_index("ctx")
    core, side, level = me % 2, (me // 2) % 2, me // 4
    head_index = lax.axis_index("head")
    rows = 2 * new_rows
    core_pairs = [(i, i ^ 1) for i in range(ctx)]
    side_pairs = [(i, i ^ 2) for i in range(ctx)]
    ring = [(i, (i + 4) % ctx) for i in range(ctx)]
    head_pairs = [(i, i ^ 1) for i in range(head)]

    def over_core(value):
        return lax.ppermute(value, "ctx", core_pairs)

    def over_side(value):
        return lax.ppermute(value, "ctx", side_pairs)

    def over_ring(value):
        return lax.ppermute(value, "ctx", ring)

    def in_order(mine, other, axis):
        first = jnp.where(core == 0, mine, other)
        second = jnp.where(core == 0, other, mine)
        return jnp.concatenate([first, second], axis=axis)

    def by_head(value, which, order):
        part = lax.dynamic_slice_in_dim(value, which * half, half, axis=1)
        return jnp.transpose(part, order)

    own = by_head(queries, core, (1, 0, 2))
    other = over_core(by_head(queries, 1 - core, (1, 0, 2)))
    slots = [in_order(own, other, 1)]
    for _ in range(depth - 1):
        slots.append(over_ring(slots[-1]))
    across = [over_side(slot) for slot in slots]

    k0 = by_head(cache_keys, core, (1, 0, 2))
    k1 = over_core(by_head(cache_keys, 1 - core, (1, 0, 2)))
    v0 = by_head(cache_values, core, (1, 2, 0))
    v1 = over_core(by_head(cache_values, 1 - core, (1, 2, 0)))
    kn = in_order(
        by_head(new_keys, core, (1, 0, 2)),
        over_core(by_head(new_keys, 1 - core, (1, 0, 2))),
        1,
    )
    fresh_values = in_order(
        by_head(new_values, core, (1, 0, 2)),
        over_core(by_head(new_values, 1 - core, (1, 0, 2))),
        1,
    )
    vn = jnp.transpose(fresh_values, (0, 2, 1))
    key_request = jnp.concatenate([cache_request, over_core(cache_request)])
    local = cache_request.shape[0]
    chunk = min(512, local)
    lanes = jnp.arange(dh, dtype=jnp.int32)[None, :]

    def key_mask(request):
        hidden = (lanes < REQUESTS) & (lanes != request[:, None])
        return jnp.where(hidden, NEG, 0.0).astype(jnp.bfloat16)

    def query_mask(request):
        return (lanes == request[:, None]).astype(jnp.bfloat16)

    chip_first = (me // 2) * rows
    fresh_request = lax.dynamic_slice_in_dim(new_request, chip_first, rows)
    km, knm = key_mask(key_request), key_mask(fresh_request)
    knpos = (chip_first + jnp.arange(rows, dtype=jnp.int32))[:, None]
    ends = key_request.reshape(-1, chunk)
    ends = jnp.stack([ends[:, 0], ends[:, -1]], axis=1).reshape(-1)

    partial = []
    for s in range(depth):
        there = (level - s + depth) % depth
        starts = [(there * 2 + side) * rows, (there * 2 + 1 - side) * rows]
        request = jnp.concatenate(
            [lax.dynamic_slice_in_dim(new_request, start, rows) for start in starts]
        )
        qpos = jnp.concatenate([start + jnp.arange(rows, dtype=jnp.int32) for start in starts])
        meta = jnp.concatenate(
            [
                jnp.stack(
                    [
                        jnp.min(request),
                        jnp.max(request),
                        jnp.max(qpos),
                        chip_first,
                        fresh_request[0],
                        fresh_request[-1],
                    ]
                ),
                ends,
            ]
        ).astype(jnp.int32)
        partial.append(
            attend(
                meta,
                slots[s],
                across[s],
                query_mask(request),
                qpos[None, :],
                k0,
                k1,
                kn,
                km,
                knm,
                knpos,
                v0,
                v1,
                vn,
                chunk,
            )
        )

    merged = [None] * depth
    for s in list(range(1, depth)) + [0]:
        merged[s] = merge(partial[s][0], over_side(partial[s][1]))
    moving = merged[1 % depth]
    for s in list(range(2, depth)) + [0]:
        moving = merge(merged[s], over_ring(moving))
    attended = jnp.transpose(moving[:, :dh, :], (2, 0, 1)).reshape(rows, half * dh)

    def rows_of(value, which, count):
        return lax.dynamic_slice_in_dim(value, which * count, count, axis=0)

    flattened = in_order(
        rows_of(attended, core, new_rows), over_core(rows_of(attended, 1 - core, new_rows)), 1
    )
    head_terms = jnp.dot(
        flattened,
        out_weight.reshape(local_heads * dh, -1),
        preferred_element_type=jnp.float32,
    )
    model_width = head_terms.shape[1]
    slice_width = patch_hidden.shape[1]

    if head == 2:

        def over_head(value):
            return lax.ppermute(value, "head", head_pairs)

        hidden_other = over_head(patch_hidden)
        hidden = jnp.where(
            head_index == 0,
            jnp.concatenate([patch_hidden, hidden_other], axis=1),
            jnp.concatenate([hidden_other, patch_hidden], axis=1),
        )
        terms_other = over_head(head_terms.astype(jnp.bfloat16))
        patch_full = (
            hidden.astype(jnp.float32) + (head_terms + terms_other.astype(jnp.float32))
        ).astype(jnp.bfloat16)
        patch_out = lax.dynamic_slice_in_dim(patch_full, head_index * slice_width, slice_width, 1)
        normed = row_norm(patch_full.astype(jnp.float32), norm_gain, 1e-05).astype(jnp.bfloat16)
    else:
        projected = lax.psum_scatter(head_terms, "head", scatter_dimension=1, tiled=True)
        patch_out = (patch_hidden.astype(jnp.float32) + projected).astype(jnp.bfloat16)
        widened = patch_out.astype(jnp.float32)
        squares = lax.psum(jnp.sum(widened * widened, axis=1), "head")
        gain_part = lax.dynamic_slice_in_dim(norm_gain, head_index * slice_width, slice_width)
        normed_part = (
            widened * lax.rsqrt(squares / model_width + 1e-05)[:, None] * gain_part
        ).astype(jnp.bfloat16)
        normed = lax.all_gather(normed_part, "head", axis=1, tiled=True)

    dec_width = dec_kv_weight.shape[2]
    dec_heads = dec_width // DEC_DH
    dec_half = dec_width // 2
    patch_proj = jnp.dot(
        normed,
        dec_kv_weight.reshape(dec_kv_weight.shape[0], 2 * dec_width),
        preferred_element_type=jnp.float32,
    )
    patch_keys = (
        row_norm(patch_proj[:, :dec_width].reshape(new_rows, dec_heads, DEC_DH), key_gain, 1e-06)
        .astype(jnp.bfloat16)
        .reshape(new_rows, dec_width)
    )
    patch_values = patch_proj[:, dec_width:].astype(jnp.bfloat16)

    def cols_of(value, which, count):
        return lax.dynamic_slice_in_dim(value, which * count, count, axis=1)

    def half_of(which):
        return jnp.concatenate(
            [cols_of(patch_keys, which, dec_half), cols_of(patch_values, which, dec_half)], axis=1
        )

    patch_slots = [in_order(half_of(core), over_core(half_of(1 - core)), 0)]
    for _ in range(depth - 1):
        patch_slots.append(over_ring(patch_slots[-1]))
    patch_across = [over_side(slot) for slot in patch_slots]
    blocks, numbers = [], []
    for s in range(depth):
        there = (level - s + depth) % depth
        blocks += [patch_slots[s], patch_across[s]]
        numbers += [there * 2 + side, there * 2 + 1 - side]

    byte_rows = byte_states.shape[0]
    query_proj = jnp.dot(byte_states, dec_query_weight, preferred_element_type=jnp.float32).reshape(
        byte_rows, dec_heads, DEC_DH
    )
    byte_query = (
        row_norm(query_proj, query_gain, 1e-06).astype(jnp.bfloat16).reshape(byte_rows, dec_width)
    )
    chip_query = in_order(
        cols_of(byte_query, core, dec_half), over_core(cols_of(byte_query, 1 - core, dec_half)), 0
    )
    chip_patch = in_order(byte_patch, over_core(byte_patch), 0)
    table = jnp.arange(new_request.shape[0], dtype=jnp.int32)
    chip_request = jnp.sum(
        jnp.where(table[None, :] == chip_patch[:, None], new_request[None, :], 0), axis=1
    )
    chip_low = jnp.sum((new_request[None, :] < chip_request[:, None]).astype(jnp.int32), axis=1)
    mixed = byte_attend(
        jnp.stack(numbers).astype(jnp.int32),
        chip_query,
        chip_low[:, None],
        chip_patch[:, None],
        blocks,
        dec_heads // 2,
    )
    byte_mixed = in_order(
        rows_of(mixed, core, byte_rows), over_core(rows_of(mixed, 1 - core, byte_rows)), 1
    )

    if head == 2:
        out_width = dec_out_weight.shape[1] // 2
        weight_other = over_head(cols_of(dec_out_weight, 1 - head_index, out_width))
        weight_own = cols_of(dec_out_weight, head_index, out_width)
        byte_sum = jnp.dot(byte_mixed, weight_own, preferred_element_type=jnp.float32) + jnp.dot(
            over_head(byte_mixed), weight_other, preferred_element_type=jnp.float32
        )
    else:
        byte_terms = jnp.dot(byte_mixed, dec_out_weight, preferred_element_type=jnp.float32)
        byte_sum = lax.psum_scatter(byte_terms, "head", scatter_dimension=1, tiled=True)
    out_width = byte_sum.shape[1]
    own_states = lax.dynamic_slice_in_dim(byte_states, head_index * out_width, out_width, 1)
    byte_out = (own_states.astype(jnp.float32) + byte_sum).astype(jnp.bfloat16)
    return (patch_out, byte_out)


def solution(mesh):
    placed = (
        P("ctx", "head"),
        P("ctx", "head", None),
        P("ctx", "head", None),
        P("ctx", "head", None),
        P("ctx", "head", None),
        P("ctx", "head", None),
        P("ctx"),
        P(),
        P("head", None, None),
        P(),
        P(None, None, "head"),
        P(None, "head"),
        P(),
        P(),
        P("head", None),
        P("ctx", None),
        P("ctx"),
    )
    return jax.shard_map(
        functools.partial(per_device, mesh.shape["ctx"], mesh.shape["head"]),
        mesh=mesh,
        in_specs=placed,
        out_specs=(P("ctx", "head"), P("ctx", "head")),
        check_vma=False,
    )
```

```python
import functools

import jax
import jax.numpy as jnp
from jax import lax
from jax.experimental import pallas as pl
from jax.experimental.pallas import tpu as pltpu
from jax.sharding import PartitionSpec as P

DEC_DH = 64
REQUESTS = 8
NEG = -float(2**100)
LOG2E = 1.4426950408889634
EXTRA = 8


def core_of():
    return lax.rem(lax.axis_index("ctx"), 2)


def row_norm(values, gain_values, epsilon):
    meansq = jnp.mean(values * values, axis=-1, keepdims=True)
    return values * lax.rsqrt(meansq + epsilon) * gain_values


def cost(flops, moved=0, exps=0):
    return pl.CostEstimate(flops=int(flops), bytes_accessed=int(moved), transcendentals=int(exps))


def store_halves(mine, theirs, both, base=0):
    half = both.shape[0] // 2
    core = core_of()

    @pl.when(core == 0)
    def _():
        mine[base : base + half] = both[:half]
        theirs[base : base + half] = both[half:]

    @pl.when(core == 1)
    def _():
        mine[base : base + half] = both[half:]
        theirs[base : base + half] = both[:half]


def fresh_kernel(queries, keys, values, mine, theirs):
    half = mine.shape[0] // 3
    for n, ref in enumerate((queries, keys, values)):
        store_halves(mine, theirs, jnp.swapaxes(ref[...], 0, 1), n * half)


def split_fresh(queries, keys, values):
    rows, heads, dh = queries.shape
    shape = jax.ShapeDtypeStruct((3 * (heads // 2), rows, dh), queries.dtype)
    return pl.pallas_call(
        fresh_kernel,
        out_shape=[shape, shape],
        cost_estimate=cost(1e7, 4 * queries.size),
        name="split_fresh",
    )(queries, keys, values)


def split_kernel(transposed, source, mine, theirs):
    both = source[...]
    if transposed:
        both = jnp.swapaxes(jnp.swapaxes(both.astype(jnp.float32), 0, 1), 1, 2)
        both = both.astype(jnp.bfloat16)
    else:
        both = jnp.swapaxes(both, 0, 1)
    store_halves(mine, theirs, both)


def split_cache(source, transposed, name):
    rows, heads, dh = source.shape
    tile = min(256, rows)
    half = heads // 2
    if transposed:
        spec = pl.BlockSpec((half, dh, tile), lambda i: (0, 0, i))
        shape = jax.ShapeDtypeStruct((half, dh, rows), source.dtype)
    else:
        spec = pl.BlockSpec((half, tile, dh), lambda i: (0, i, 0))
        shape = jax.ShapeDtypeStruct((half, rows, dh), source.dtype)
    return pl.pallas_call(
        functools.partial(split_kernel, transposed),
        grid=(rows // tile,),
        in_specs=[pl.BlockSpec((tile, heads, dh), lambda i: (i, 0, 0))],
        out_specs=[spec, spec],
        out_shape=[shape, shape],
        cost_estimate=cost(4e7, 4 * source.size),
        name=name,
    )(source)


def pieces_of(value):
    high = value.astype(jnp.bfloat16)
    rest = value - high.astype(jnp.float32)
    middle = rest.astype(jnp.bfloat16)
    low = (rest - middle.astype(jnp.float32)).astype(jnp.bfloat16)
    zeros = jnp.zeros((EXTRA - 3,) + value.shape[1:], jnp.bfloat16)
    return jnp.concatenate([high, middle, low, zeros], axis=0)


def attention_kernel(
    slot,
    depth,
    scale,
    new_request,
    key_request,
    q0,
    q1,
    qmask,
    k0,
    k1,
    kmask,
    ka,
    kb,
    nmask,
    v0,
    v1,
    va,
    vb,
    out0,
    out1,
    m_ref,
    l_ref,
    acc_ref,
):
    group, rows, dh = q0.shape
    local = k0.shape[1]
    me = lax.axis_index("ctx")
    core, side, level = lax.rem(me, 2), lax.rem(me // 2, 2), me // 4
    there = lax.rem(level - slot + depth, depth)
    chips = (there * 2 + side, there * 2 + 1 - side)
    first = there * 2 * rows
    q_low, q_high = new_request[first], new_request[first + 2 * rows - 1]
    own = (level * 2 + side) * rows
    n_low, n_high = new_request[own], new_request[own + rows - 1]

    queries = []
    masks = [qmask[pl.ds(pl.multiple_of(chip * rows, rows), rows), :] for chip in chips]
    mask = jnp.concatenate(masks, axis=0)
    for h in range(group):
        both = jnp.concatenate([q0[h], q1[h]], axis=0)
        queries.append(jnp.concatenate([both, mask], axis=1))
    m_ref[...] = jnp.full(m_ref.shape, 2.0 * NEG, jnp.float32)
    l_ref[...] = jnp.zeros(l_ref.shape, jnp.float32)
    acc_ref[...] = jnp.zeros(acc_ref.shape, jnp.float32)

    def scores_of(h, keys, hidden):
        return lax.dot_general(
            jnp.concatenate([keys, hidden], axis=1),
            queries[h],
            (((1,), (1,)), ((), ())),
            preferred_element_type=jnp.float32,
        )

    def step(h, scores, values, dims):
        before = m_ref[h]
        now = jnp.maximum(before, jnp.max(scores, axis=0, keepdims=True))
        weights = jnp.exp2((scores - now) * scale)
        keep = jnp.exp2((before - now) * scale)
        m_ref[h] = now
        l_ref[h] = l_ref[h] * keep + jnp.sum(weights, axis=0, keepdims=True)
        mixed = lax.dot_general(
            values,
            weights.astype(jnp.bfloat16),
            (dims, ((), ())),
            preferred_element_type=jnp.float32,
        )
        acc_ref[h] = acc_ref[h] * keep + mixed

    for which, (kref, vref) in enumerate(((k0, v0), (k1, v1))):
        low, high = key_request[which * local], key_request[which * local + local - 1]

        @pl.when((low <= q_high) & (high >= q_low))
        def _():
            hidden = kmask[which * local : (which + 1) * local, :]
            scores = [scores_of(h, kref[h], hidden) for h in range(group)]
            for h in range(group):
                step(h, scores[h], vref[h], ((1,), (0,)))

    @pl.when((n_low <= q_high) & (n_high >= q_low) & (own < first + 2 * rows))
    def _():
        hidden = nmask[pl.ds(pl.multiple_of(own, rows), rows), :]
        fresh = rows // 2
        flip = core * fresh
        kpos = own + (lax.broadcasted_iota(jnp.int32, (rows, rows), 0) ^ flip)
        lane = lax.broadcasted_iota(jnp.int32, (rows, rows), 1) ^ flip
        seen = jnp.concatenate([kpos <= chip * rows + lane for chip in chips], axis=1)
        for h in range(group):
            keys = jnp.concatenate([ka[h], kb[h]], axis=0)
            values = jnp.concatenate([va[h], vb[h]], axis=0)
            scores = jnp.where(seen, scores_of(h, keys, hidden), NEG)
            step(h, scores, values, ((0,), (0,)))

    for h in range(group):
        total = l_ref[h]
        total = jnp.where(total == 0.0, 1.0, total)
        mixed = (acc_ref[h] / total).astype(jnp.bfloat16)
        extra = pieces_of(m_ref[h] * scale + jnp.log2(total))
        for d, out in enumerate((out0, out1)):
            at = slice(d * rows, (d + 1) * rows)
            out[h, :dh, :] = mixed[:, at]
            out[h, dh:, :] = extra[:, at]


def attend(slot, depth, requests, q0, q1, masks, k0, k1, v0, v1, fresh_own, fresh_other):
    heads, rows, dh = q0.shape
    scale = dh ** (-0.5) * LOG2E
    local, fresh = k0.shape[1], fresh_own.shape[1]
    group = 2 if heads % 2 == 0 else 1
    qmask, kmask, nmask = masks

    def per_head(*shape, base=0):
        return pl.BlockSpec((group,) + shape, lambda h, *_: (h + base // group, 0, 0))

    def whole(array):
        return pl.BlockSpec(array.shape, lambda h, *_: (0,) * array.ndim)

    shape = jax.ShapeDtypeStruct((heads, dh + EXTRA, rows), jnp.bfloat16)
    return pl.pallas_call(
        functools.partial(attention_kernel, slot, depth, scale),
        grid_spec=pltpu.PrefetchScalarGridSpec(
            num_scalar_prefetch=2,
            grid=(heads // group,),
            in_specs=[
                per_head(rows, dh),
                per_head(rows, dh),
                whole(qmask),
                per_head(local, dh),
                per_head(local, dh),
                whole(kmask),
                per_head(fresh, dh, base=heads),
                per_head(fresh, dh, base=heads),
                whole(nmask),
                per_head(dh, local),
                per_head(dh, local),
                per_head(fresh, dh, base=2 * heads),
                per_head(fresh, dh, base=2 * heads),
            ],
            out_specs=[per_head(dh + EXTRA, rows)] * 2,
            scratch_shapes=[
                pltpu.VMEM((group, 1, 2 * rows), jnp.float32),
                pltpu.VMEM((group, 1, 2 * rows), jnp.float32),
                pltpu.VMEM((group, dh, 2 * rows), jnp.float32),
            ],
        ),
        out_shape=[shape, shape],
        cost_estimate=cost(
            16 * heads * rows * local * dh, 8 * heads * local * dh, 4 * heads * rows * local
        ),
        name="attend",
    )(
        *requests,
        q0,
        q1,
        qmask,
        k0,
        k1,
        kmask,
        fresh_own,
        fresh_other,
        nmask,
        v0,
        v1,
        fresh_own,
        fresh_other,
    )


def merge_kernel(final, *refs):
    parts, outs = (refs[:-2], refs[-2:]) if final else (refs[:-1], refs[-1:])
    heads, height, rows = parts[0].shape
    dh = height - EXTRA
    for h in range(heads):
        sums = [
            jnp.sum(p[h, dh : dh + 3, :].astype(jnp.float32), axis=0, keepdims=True) for p in parts
        ]
        top = functools.reduce(jnp.maximum, sums)
        shares = [jnp.exp2(s - top) for s in sums]
        total = functools.reduce(jnp.add, shares)
        scale = 1.0 / total
        mixed = functools.reduce(
            jnp.add,
            [p[h, :dh, :].astype(jnp.float32) * (w * scale) for p, w in zip(parts, shares)],
        )
        if final:
            mine, theirs = outs
            flat = mixed.T.astype(jnp.bfloat16)
            mine[:, h * dh : (h + 1) * dh] = flat[: rows // 2]
            theirs[:, h * dh : (h + 1) * dh] = flat[rows // 2 :]
        else:
            outs[0][h, :dh, :] = mixed.astype(jnp.bfloat16)
            outs[0][h, dh:, :] = pieces_of(top + jnp.log2(total))


def merge(*parts, final=False):
    heads, height, rows = parts[0].shape
    if final:
        flat = jax.ShapeDtypeStruct((rows // 2, heads * (height - EXTRA)), jnp.bfloat16)
        shapes = [flat, flat]
    else:
        shapes = [jax.ShapeDtypeStruct(parts[0].shape, parts[0].dtype)]
    outs = pl.pallas_call(
        functools.partial(merge_kernel, final),
        out_shape=shapes,
        cost_estimate=cost(3e6, 2 * (len(parts) + 1) * parts[0].size),
        name="merge",
    )(*parts)
    return outs if final else outs[0]


def project_kernel(mine, other, weight, out, short):
    width = mine.shape[1]
    core = core_of()
    at = pl.ds(pl.multiple_of(core * width, width), width)
    off = pl.ds(pl.multiple_of((1 - core) * width, width), width)
    terms = jnp.dot(mine[...], weight[at, :], preferred_element_type=jnp.float32)
    terms += jnp.dot(other[...], weight[off, :], preferred_element_type=jnp.float32)
    out[...] = terms
    short[...] = terms.astype(jnp.bfloat16)


def project(mine, other, weight, first, width):
    rows, half = mine.shape
    tile = min(512, width)
    whole = pl.BlockSpec((rows, half), lambda i: (0, 0))
    out = pl.BlockSpec((rows, tile), lambda i: (0, i))
    return pl.pallas_call(
        project_kernel,
        grid=(width // tile,),
        in_specs=[
            whole,
            whole,
            pl.BlockSpec((2 * half, tile), lambda i: (0, i + first // tile)),
        ],
        out_specs=[out, out],
        out_shape=[
            jax.ShapeDtypeStruct((rows, width), jnp.float32),
            jax.ShapeDtypeStruct((rows, width), jnp.bfloat16),
        ],
        cost_estimate=cost(4 * rows * half * width, 4 * half * width),
        name="project",
    )(mine, other, weight)


def head_norm(values, gain, width):
    parts = []
    for h in range(width // DEC_DH):
        part = values[:, h * DEC_DH : (h + 1) * DEC_DH]
        parts.append(row_norm(part, gain, 1e-06))
    return jnp.concatenate(parts, axis=1)


def store_columns(mine, theirs, values, base):
    half = values.shape[1] // 2
    core = core_of()

    @pl.when(core == 0)
    def _():
        mine[:, base : base + half] = values[:, :half]
        theirs[:, base : base + half] = values[:, half:]

    @pl.when(core == 1)
    def _():
        mine[:, base : base + half] = values[:, half:]
        theirs[:, base : base + half] = values[:, :half]


def patch_kernel(chunks, joined, *refs):
    if joined:
        terms = refs[:chunks]
        others = refs[chunks : 2 * chunks]
        hidden, hidden_other, gain, key_gain, weight = refs[2 * chunks : 2 * chunks + 5]
        patch_out, mine, theirs, normed, acc = refs[2 * chunks + 5 :]
    else:
        rows_in, key_gain, weight, mine, theirs, normed, acc = refs
    step = pl.program_id(0)

    @pl.when(step == 0)
    def _():
        acc[...] = jnp.zeros(acc.shape, jnp.float32)
        if joined:
            total = jnp.concatenate([t[...] for t in terms], axis=1)
            total += jnp.concatenate([t[...].astype(jnp.float32) for t in others], axis=1)
            half = hidden.shape[1]
            first = lax.axis_index("head") == 0
            near, far = hidden[...].astype(jnp.float32), hidden_other[...].astype(jnp.float32)
            left = jnp.where(first, near, far) + total[:, :half]
            right = jnp.where(first, far, near) + total[:, half:]
            full = jnp.concatenate([left, right], axis=1).astype(jnp.bfloat16)
            patch_out[...] = jnp.where(first, full[:, :half], full[:, half:])
            result = row_norm(full.astype(jnp.float32), gain[...], 1e-05).astype(jnp.bfloat16)
        else:
            result = rows_in[...]
        for n in range(normed.shape[0]):
            normed[n] = result[:, n * normed.shape[2] : (n + 1) * normed.shape[2]]

    for part in range(2):
        width = weight.shape[2]
        acc[part] += jnp.dot(normed[step], weight[part], preferred_element_type=jnp.float32)

    @pl.when(step == pl.num_programs(0) - 1)
    def _():
        width = weight.shape[2]
        keys = head_norm(acc[0], key_gain[...], width).astype(jnp.bfloat16)
        store_columns(mine, theirs, keys, 0)
        store_columns(mine, theirs, acc[1].astype(jnp.bfloat16), width // 2)


def patch_rows(terms, others, hidden, hidden_other, gain, key_gain, weight, rows_in=None):
    joined = rows_in is None
    _, model, width = weight.shape
    tile = min(1024, model)
    operands = (
        list(terms) + list(others) + [hidden, hidden_other, gain] if joined else [rows_in]
    ) + [key_gain]
    rows = operands[0].shape[0]

    def whole(array):
        return pl.BlockSpec(array.shape, lambda i: (0,) * array.ndim)

    half = jax.ShapeDtypeStruct((rows, width), jnp.bfloat16)
    shapes = ([jax.ShapeDtypeStruct(hidden.shape, jnp.bfloat16)] if joined else []) + [half, half]
    return pl.pallas_call(
        functools.partial(patch_kernel, len(terms), joined),
        grid=(model // tile,),
        in_specs=[whole(a) for a in operands]
        + [pl.BlockSpec((2, tile, width), lambda i: (0, i, 0))],
        out_specs=[whole(s) for s in shapes],
        out_shape=shapes,
        scratch_shapes=[
            pltpu.VMEM((model // tile, rows, tile), jnp.bfloat16),
            pltpu.VMEM((2, rows, width), jnp.float32),
        ],
        cost_estimate=cost(4 * rows * model * width, 4 * model * width),
        name="patch_rows",
    )(*operands, weight)


def byte_query_kernel(states, weight, gain, mine, theirs):
    terms = jnp.dot(states[...], weight[...], preferred_element_type=jnp.float32)
    values = head_norm(terms, gain[...], terms.shape[1]).astype(jnp.bfloat16)
    store_columns(mine, theirs, values, 0)


def byte_queries(states, weight, gain):
    rows, width = states.shape[0], weight.shape[1]
    half = jax.ShapeDtypeStruct((rows, width // 2), jnp.bfloat16)
    return pl.pallas_call(
        byte_query_kernel,
        out_shape=[half, half],
        cost_estimate=cost(2 * states.size * width, 2 * states.size),
        name="byte_queries",
    )(states, weight, gain)


def byte_kernel(heads, depth, query_a, query_b, low_a, high_a, low_b, high_b, *refs):
    blocks = refs[:-2]
    rows = blocks[0].shape[0]
    width = heads * DEC_DH
    me = lax.axis_index("ctx")
    core, side, level = lax.rem(me, 2), lax.rem(me // 2, 2), me // 4
    lane = lax.broadcasted_iota(jnp.int32, (1, rows), 1) ^ (core * (rows // 2))
    numbers = []
    for slot in range(depth):
        there = lax.rem(level - slot + depth, depth)
        numbers += [there * 2 + side, there * 2 + 1 - side]
    position = jnp.concatenate([lane + number * rows for number in numbers], axis=1)
    for query, low, high, out in (
        (query_a, low_a, high_a, refs[-2]),
        (query_b, low_b, high_b, refs[-1]),
    ):
        seen = (position >= low[...]) & (position <= high[...])
        for h in range(heads):
            at = slice(h * DEC_DH, (h + 1) * DEC_DH)
            vat = slice(width + h * DEC_DH, width + (h + 1) * DEC_DH)
            keys = jnp.concatenate([b[:, at] for b in blocks], axis=0)
            values = jnp.concatenate([b[:, vat] for b in blocks], axis=0)
            scores = lax.dot_general(
                query[:, at], keys, (((1,), (1,)), ((), ())), preferred_element_type=jnp.float32
            )
            weights = jnp.where(seen, jnp.exp2(scores * (DEC_DH ** (-0.5) * LOG2E)), 0.0)
            total = jnp.sum(weights, axis=1, keepdims=True)
            mixed = jnp.dot(
                weights.astype(jnp.bfloat16), values, preferred_element_type=jnp.float32
            )
            out[:, at] = (mixed / total).astype(jnp.bfloat16)


def byte_attend(depth, queries, bounds, blocks):
    rows, width = queries[0].shape
    shape = jax.ShapeDtypeStruct((rows, width), jnp.bfloat16)
    keys = len(blocks) * blocks[0].shape[0]
    return pl.pallas_call(
        functools.partial(byte_kernel, width // DEC_DH, depth),
        out_shape=[shape, shape],
        cost_estimate=cost(8 * rows * keys * width, 8 * keys * width, 2 * rows * keys),
        name="byte_attend",
    )(*queries, *bounds, *blocks)


def per_device(
    ctx,
    head,
    patch_hidden,
    queries,
    new_keys,
    new_values,
    cache_keys,
    cache_values,
    cache_request,
    new_request,
    out_weight,
    norm_gain,
    dec_kv_weight,
    dec_query_weight,
    query_gain,
    key_gain,
    dec_out_weight,
    byte_states,
    byte_patch,
):
    new_rows, local_heads, dh = queries.shape
    depth = ctx // 4
    half = local_heads // 2
    core = core_of()
    head_index = lax.axis_index("head")
    rows = 2 * new_rows
    core_pairs = [(i, i ^ 1) for i in range(ctx)]
    side_pairs = [(i, i ^ 2) for i in range(ctx)]
    ring = [(i, (i + 4) % ctx) for i in range(ctx)]
    head_pairs = [(i, i ^ 1) for i in range(head)]

    def over_core(value):
        return lax.ppermute(value, "ctx", core_pairs)

    def over_side(value):
        return lax.ppermute(value, "ctx", side_pairs)

    def over_ring(value):
        return lax.ppermute(value, "ctx", ring)

    def over_head(value):
        return lax.ppermute(value, "head", head_pairs)

    def cols_of(value, which, count):
        return lax.dynamic_slice_in_dim(value, which * count, count, axis=1)

    fresh_own, fresh_theirs = split_fresh(queries, new_keys, new_values)
    fresh_other = over_core(fresh_theirs)
    slots = [jnp.concatenate([fresh_own[:half], fresh_other[:half]], axis=1)]

    slots[0], cache_keys = lax.optimization_barrier((slots[0], cache_keys))
    for _ in range(depth - 1):
        slots.append(over_ring(slots[-1]))
    across = [over_side(slot) for slot in slots]
    k0, theirs = split_cache(cache_keys, False, "split_keys")
    k1 = over_core(theirs)
    k1, cache_values = lax.optimization_barrier((k1, cache_values))
    v0, theirs = split_cache(cache_values, True, "split_values")
    v1 = over_core(theirs)

    lanes = jnp.arange(dh, dtype=jnp.int32)[None, :]

    def key_mask(request):
        hidden = (lanes < REQUESTS) & (lanes != request[:, None])
        return jnp.where(hidden, NEG, 0.0).astype(jnp.bfloat16)

    pairs = new_request.reshape(-1, 2, new_rows)
    swapped = jnp.where(core == 0, pairs, pairs[:, ::-1]).reshape(-1)
    key_request = jnp.concatenate([cache_request, over_core(cache_request)])
    masks = (
        (lanes == swapped[:, None]).astype(jnp.bfloat16),
        key_mask(key_request),
        key_mask(swapped),
    )

    byte_rows = byte_states.shape[0]
    byte_own, byte_theirs = byte_queries(byte_states, dec_query_weight, query_gain[None, :])
    byte_other = over_core(byte_theirs)
    table = jnp.arange(new_request.shape[0], dtype=jnp.int32)
    byte_request = jnp.sum(
        jnp.where(table[None, :] == byte_patch[:, None], new_request[None, :], 0), axis=1
    )
    byte_low = jnp.sum((new_request[None, :] < byte_request[:, None]).astype(jnp.int32), axis=1)
    bounds_own = jnp.stack([byte_low, byte_patch])
    bounds_other = over_core(bounds_own)
    bounds = [b[n][:, None] for b in (bounds_own, bounds_other) for n in range(2)]
    dec_width = dec_kv_weight.shape[2]
    kv_weight = jnp.transpose(dec_kv_weight, (1, 0, 2))

    def relative(weight):
        first, second = weight[: dec_width // 2], weight[dec_width // 2 :]
        return jnp.where(
            core == 0, weight, jnp.concatenate([second, first], axis=0)
        )

    early = [byte_own, byte_other] + bounds + [kv_weight]
    if head == 2:
        out_width = dec_out_weight.shape[1] // 2
        weight_other = over_head(relative(cols_of(dec_out_weight, 1 - head_index, out_width)))
        weight_own = relative(cols_of(dec_out_weight, head_index, out_width))
        hidden_other = over_head(patch_hidden)
        early += [weight_other, weight_own, hidden_other]
    else:
        weight_own = relative(dec_out_weight)
    tied = lax.optimization_barrier(tuple(early) + (v1,))
    early, v1 = tied[:-1], tied[-1]
    byte_own, byte_other, *bounds = early[:6]
    kv_weight = early[6]
    if head == 2:
        weight_other, weight_own, hidden_other = early[7:]

    partial = [None] * depth
    order = list(range(1, depth)) + [0]
    for s in order:
        partial[s] = attend(
            s,
            depth,
            (new_request, key_request),
            slots[s],
            across[s],
            masks,
            k0,
            k1,
            v0,
            v1,
            fresh_own,
            fresh_other,
        )

    moving = []
    for s in order:
        parts = [partial[s][0], over_side(partial[s][1])] + moving
        if s:
            moving = [over_ring(merge(*parts))]
        else:
            attended, attended_theirs = merge(*parts, final=True)
    attended_other = over_core(attended_theirs)

    weight = out_weight.reshape(local_heads * dh, -1)
    model_width = weight.shape[1]
    slice_width = patch_hidden.shape[1]
    if head == 2:
        terms, others = [], []
        chunk = model_width // 2
        for n in range(2):
            full, short = project(attended, attended_other, weight, n * chunk, chunk)
            terms.append(full)
            others.append(over_head(short))
        patch_out, patch_own, patch_theirs = patch_rows(
            terms,
            others,
            patch_hidden,
            hidden_other,
            norm_gain[None, :],
            key_gain[None, :],
            kv_weight,
        )
    else:
        head_terms, _ = project(attended, attended_other, weight, 0, model_width)
        projected = lax.psum_scatter(head_terms, "head", scatter_dimension=1, tiled=True)
        patch_out = (patch_hidden.astype(jnp.float32) + projected).astype(jnp.bfloat16)
        widened = patch_out.astype(jnp.float32)
        squares = lax.psum(jnp.sum(widened * widened, axis=1), "head")
        gain_part = lax.dynamic_slice_in_dim(norm_gain, head_index * slice_width, slice_width)
        normed_part = (
            widened * lax.rsqrt(squares / model_width + 1e-05)[:, None] * gain_part
        ).astype(jnp.bfloat16)
        normed = lax.all_gather(normed_part, "head", axis=1, tiled=True)
        patch_own, patch_theirs = patch_rows(
            [], [], None, None, None, key_gain[None, :], kv_weight, normed
        )

    patch_slots = [jnp.concatenate([patch_own, over_core(patch_theirs)], axis=0)]
    for _ in range(depth - 1):
        patch_slots.append(over_ring(patch_slots[-1]))
    blocks = []
    for slot in patch_slots:
        blocks += [slot, over_side(slot)]

    mixed_own, mixed_theirs = byte_attend(depth, (byte_own, byte_other), bounds, blocks)
    byte_mixed = jnp.concatenate([mixed_own, over_core(mixed_theirs)], axis=1)
    if head == 2:
        byte_sum = jnp.dot(byte_mixed, weight_own, preferred_element_type=jnp.float32) + jnp.dot(
            over_head(byte_mixed), weight_other, preferred_element_type=jnp.float32
        )
    else:
        byte_terms = jnp.dot(byte_mixed, weight_own, preferred_element_type=jnp.float32)
        byte_sum = lax.psum_scatter(byte_terms, "head", scatter_dimension=1, tiled=True)
    out_width = byte_sum.shape[1]
    own_states = lax.dynamic_slice_in_dim(byte_states, head_index * out_width, out_width, 1)
    byte_out = (own_states.astype(jnp.float32) + byte_sum).astype(jnp.bfloat16)
    return (patch_out, byte_out)


def solution(mesh):
    placed = (
        P("ctx", "head"),
        P("ctx", "head", None),
        P("ctx", "head", None),
        P("ctx", "head", None),
        P("ctx", "head", None),
        P("ctx", "head", None),
        P("ctx"),
        P(),
        P("head", None, None),
        P(),
        P(None, None, "head"),
        P(None, "head"),
        P(),
        P(),
        P("head", None),
        P("ctx", None),
        P("ctx"),
    )
    return jax.shard_map(
        functools.partial(per_device, mesh.shape["ctx"], mesh.shape["head"]),
        mesh=mesh,
        in_specs=placed,
        out_specs=(P("ctx", "head"), P("ctx", "head")),
        check_vma=False,
    )
```
